32 devices in a mesh: prompt: 2 (over y), seq: 2 (over x), blk: 4 (over z), cfg: 2 (over core).
Axes of the slice: x: 2, y: 2, z: 4, core: 2. Of those that a mesh axis runs over, the one named last changes fastest.
Arguments:
- queries: bfloat16 [2, 384, 4096], P('cfg', ('prompt', 'blk', 'seq')), parts along dimension 1, may hold values from -5 to 5
- key_states: bfloat16 [2, 384, 4096], P('cfg', ('prompt', 'blk', 'seq')), parts along dimension 1, may hold values from -5 to 5
- value_states: bfloat16 [2, 384, 4096], P('cfg', ('prompt', 'blk', 'seq')), parts along dimension 1, may hold values from -6 to 6
- noisy_latents: float32 [384, 64], P(('prompt', 'blk', 'seq')), parts along dimension 0, may hold values from -6 to 6
- patch_order: int32 [384], P(('prompt', 'blk', 'seq')), parts along dimension 0, may hold values from 0 to 191, as said below
- head_weight: bfloat16 [4096, 64], replicated, may hold values from -0.75 to 0.75
- latent_std: float32 [16], replicated, may hold values from 0.1 to 1.9
- latent_mean: float32 [16], replicated, may hold values from -3 to 3
- conv_weight: bfloat16 [3, 3, 3, 16, 384], replicated, may hold values from -0.3125 to 0.3125
- conv_bias: float32 [384], replicated, may hold values from -2 to 2
Outputs:
- features: bfloat16 [8, 8, 24, 384], P(('prompt', 'cfg'), 'seq', 'blk'), parts along dimension 0
The draws below stay inside these ranges and needn't reach their ends.
There are 2 independent parts, one for each index of `prompt`. The reference program is written for one: setup_inputs(seed, part) draws one part's arguments, and reference() takes and returns one part's arrays. A program takes and returns all parts, laid end to end along the dimension named above; an argument that names none is the same for every part. Nothing has to cross between parts.
Inputs may be any that keep to these rules, and one draw needn't show every extreme that they name: A permutation of 0 to 191 that keeps every aligned block of 24 tokens within itself: patch_order[t] // 24 == t // 24.
All inputs are finite; a program needn't handle non-finite values.
Results may differ from the reference program's by a relative error of at most 0.012.
Values may be sent and summed in bfloat16 or wider, within the bound.
No kernel may reach another device: no remote copies, remote signals or barrier semaphores. Data moves between devices by JAX's collectives and lax.ppermute only.
A program may use at most 128 MiB of HBM per device.

```python
import math
import jax
import jax.numpy as jnp
from jax import lax

HEADS = 32
HDIM = 128
ZCH = 16
CONV_OUT = 384
PATCH = 64
HD = 4096
FRAMES = 4
HP = 4
WP = 12
TOK_DEV = 24
TOKENS = 192


def attention_pair(key):
    base = jax.random.fold_in(key, 7)
    key_query, key_keys = jax.random.split(base, 2)
    shape = (2, TOKENS, HEADS * HDIM)
    query_part = jax.random.truncated_normal(key_query, -4.0, 4.0, shape, jnp.float32)
    keys_part = jax.random.truncated_normal(key_keys, -4.0, 4.0, shape, jnp.float32)
    return (query_part, keys_part)


def draw_queries(key, part):
    return attention_pair(key)[0].astype(jnp.bfloat16)


def draw_key_states(key, part):
    return attention_pair(key)[1].astype(jnp.bfloat16)


def draw_patch_order(key, part):
    blocks = TOKENS // TOK_DEV
    subkeys = jax.random.split(jax.random.fold_in(key, 11), blocks)
    orders = jax.vmap(lambda single: jax.random.permutation(single, TOK_DEV))(subkeys)
    offsets = (jnp.arange(blocks, dtype=jnp.int32) * TOK_DEV)[:, None]
    return (orders.astype(jnp.int32) + offsets).reshape(TOKENS).astype(jnp.int32)


def shard_levels(rng, extent, cuts, low, top_value):
    gain, own = 1.0, jax.random.fold_in(rng, 6)
    for axis_at, blocks in cuts:
        draws = jnp.exp(jax.random.uniform(jax.random.fold_in(own, axis_at), (blocks,), jnp.float32, low / len(cuts), top_value / len(cuts)))
        gain = gain * jnp.repeat(draws, extent[axis_at] // blocks).reshape([-1 if axis == axis_at else 1 for axis in range(len(extent))])
    return gain


def normal_values(stream_key, dims, scale, bound, cuts=(), kind=jnp.bfloat16):
    entries = scale * jax.random.normal(stream_key, dims, jnp.float32)
    if cuts:
        entries = entries * shard_levels(stream_key, dims, cuts, -0.22, 0.18)
    return jnp.clip(entries, -bound, bound).astype(kind)


def setup_inputs(seed: int = 0, part: int = 0) -> dict:
    arg_keys = jax.random.split(jax.random.key(seed), 11)
    part_splits = jax.random.split(jax.random.fold_in(arg_keys[10], part), 11)
    queries = draw_queries(jax.random.fold_in(jax.random.fold_in(arg_keys[10], part), 71), part)
    key_states = draw_key_states(jax.random.fold_in(jax.random.fold_in(arg_keys[10], part), 71), part)
    value_states = normal_values(part_splits[2], (2, TOKENS, HD), 1.0, 6.0, ((0, 2), (1, 8)))
    noisy_latents = normal_values(part_splits[3], (TOKENS, PATCH), 1.0, 6.0, ((0, 8),), jnp.float32)
    patch_order = draw_patch_order(jax.random.fold_in(jax.random.fold_in(arg_keys[10], part), 71), part)
    head_weight = normal_values(arg_keys[5], (HD, PATCH), (HD // 64) ** -0.5, 0.75)
    latent_std = jnp.clip(1.0 + 0.18 * jax.random.normal(arg_keys[6], (ZCH,), jnp.float32), 0.1, 1.9)
    latent_mean = normal_values(arg_keys[7], (ZCH,), 0.5, 3.0, (), jnp.float32)
    conv_weight = normal_values(arg_keys[8], (3, 3, 3, ZCH, CONV_OUT), (27 * ZCH) ** -0.5, 0.3125)
    conv_bias = normal_values(arg_keys[9], (CONV_OUT,), 0.3, 2.0, (), jnp.float32)
    return {"queries": queries, "key_states": key_states, "value_states": value_states, "noisy_latents": noisy_latents, "patch_order": patch_order, "head_weight": head_weight, "latent_std": latent_std, "latent_mean": latent_mean, "conv_weight": conv_weight, "conv_bias": conv_bias}


GUIDE = 5.0
NOISE_LEVEL = 0.5

def reference(queries, key_states, value_states, noisy_latents, patch_order, head_weight, latent_std, latent_mean, conv_weight, conv_bias):
    scale = 1.0 / math.sqrt(HDIM)

    def one_head(index):
        branch = (index // HEADS).astype(jnp.int32)
        head = (index % HEADS).astype(jnp.int32)
        start = (jnp.int32(0) * branch, jnp.int32(0) * branch, head * HDIM)
        q_rows = lax.dynamic_slice(queries, (branch, start[1], start[2]), (1, TOKENS, HDIM))[0]
        k_rows = lax.dynamic_slice(key_states, (branch, start[1], start[2]), (1, TOKENS, HDIM))[0]
        v_rows = lax.dynamic_slice(value_states, (branch, start[1], start[2]), (1, TOKENS, HDIM))[0]
        scores = jnp.dot(q_rows, k_rows.T, preferred_element_type=jnp.float32) * scale
        top = lax.optimization_barrier(jnp.max(scores, axis=1, keepdims=True))
        expo = jnp.exp(scores - top)
        total = lax.optimization_barrier(jnp.sum(expo, axis=1, keepdims=True))
        mixed = jnp.dot(expo.astype(jnp.bfloat16), v_rows, preferred_element_type=jnp.float32) / total
        return mixed.astype(jnp.bfloat16)
    heads_out = lax.map(one_head, jnp.arange(2 * HEADS, dtype=jnp.int32))
    attended = heads_out.reshape(2, HEADS, TOKENS, HDIM).transpose(0, 2, 1, 3).reshape(2, TOKENS, HD)
    cond = jnp.dot(attended[0], head_weight, preferred_element_type=jnp.float32)
    uncond = jnp.dot(attended[1], head_weight, preferred_element_type=jnp.float32)
    guided = uncond + GUIDE * (cond - uncond)
    denoised = noisy_latents - NOISE_LEVEL * guided
    pixels = (denoised * jnp.tile(latent_std, 4) + jnp.tile(latent_mean, 4)).astype(jnp.bfloat16)
    placed = jnp.zeros((TOKENS, PATCH), jnp.bfloat16).at[patch_order.astype(jnp.int32)].set(pixels)
    latent_grid = placed.reshape(FRAMES, HP, WP, 2, 2, ZCH).transpose(0, 1, 3, 2, 4, 5).reshape(FRAMES, 2 * HP, 2 * WP, ZCH)
    padded = jnp.pad(latent_grid, ((2, 0), (1, 1), (1, 1), (0, 0)))
    output = jnp.zeros((FRAMES * 2 * HP * 2 * WP, CONV_OUT), jnp.float32)
    for step_t in range(3):
        for step_y in range(3):
            for step_x in range(3):
                window = padded[step_t:step_t + FRAMES, step_y:step_y + 2 * HP, step_x:step_x + 2 * WP, :]
                output = output + jnp.dot(window.reshape(-1, ZCH), conv_weight[step_t, step_y, step_x], preferred_element_type=jnp.float32)
    output = output + conv_bias[None, :]
    return output.reshape(FRAMES, 2 * HP, 2 * WP, CONV_OUT).astype(jnp.bfloat16)
```

```python
import math

import jax
import jax.numpy as jnp
import numpy as np
from jax import lax
from jax.experimental import pallas as pl
from jax.experimental.pallas import tpu as pltpu
from jax.sharding import PartitionSpec as P

HDIM = 128
ZCH = 16
COLS_DEV = 3


GUIDE = 5.0
NOISE_LEVEL = 0.5


def partner(array, axis, apart):
    return lax.ppermute(array, axis, [(i, i ^ 1 << apart) for i in range(lax.axis_size(axis))])


def padded(array, sides, width):
    for axis, dim in sides:
        devices, length = (lax.axis_size(axis), array.shape[dim])
        up = [(i, (i + 1) % devices) for i in range(devices - 1)]
        down = [(j, i) for i, j in up]
        last = lax.slice_in_dim(array, length - width, length, axis=dim)
        first = lax.slice_in_dim(array, 0, width, axis=dim)
        before = lax.ppermute(last, axis, up)
        after = lax.ppermute(first, axis, down)
        array = jnp.concatenate([before, array, after], axis=dim)
    return array


def fold_keys(carry, piece, grouped, block):
    keys_piece, values_piece = piece
    heads = grouped.shape[1]
    count = keys_piece.shape[0] // block
    key_blocks = keys_piece.reshape(count, block, heads, HDIM)
    value_blocks = values_piece.reshape(count, block, heads, HDIM)
    scale = 1.0 / math.sqrt(HDIM)

    def one_block(state, pair):
        top, total, acc = state
        key_block, value_block = pair
        scores = (
            jnp.einsum("qhd,khd->hqk", grouped, key_block, preferred_element_type=jnp.float32)
            * scale
        )
        new_top = jnp.maximum(top, jnp.max(scores, axis=2))
        expo = jnp.exp(scores - new_top[:, :, None])
        factor = jnp.exp(top - new_top)
        total = total * factor + jnp.sum(expo, axis=2)
        weights = expo.astype(jnp.bfloat16)
        update = jnp.einsum(
            "hqk,khd->qhd", weights, value_block, preferred_element_type=jnp.float32
        )
        acc = acc * factor.T[:, :, None] + update
        return ((new_top, total, acc), None)

    state, unused = lax.scan(one_block, carry, (key_blocks, value_blocks))
    return state


def start_for(rows, heads):
    return (
        jnp.full((heads, rows), -1e30, jnp.float32),
        jnp.zeros((heads, rows), jnp.float32),
        jnp.zeros((rows, heads, HDIM), jnp.float32),
    )


def finish(state):
    top, total, acc = state
    rows = acc.shape[0]
    return (acc / total.T[:, :, None]).astype(jnp.bfloat16).reshape(rows, acc.shape[1] * HDIM)


def local(
    queries,
    key_states,
    value_states,
    noisy_latents,
    patch_order,
    head_weight,
    latent_std,
    latent_mean,
    conv_weight,
    conv_bias,
):
    seq_count = lax.axis_size("seq")
    blk_count = lax.axis_size("blk")
    seq_index = lax.axis_index("seq")
    blk_index = lax.axis_index("blk")
    cfg_index = lax.axis_index("cfg")
    tok_rows = queries.shape[1]
    own_query = queries[0]
    own_keys = key_states[0]
    own_values = value_states[0]
    local_query, local_keys, local_values = (
        lax.all_to_all(own_query, "seq", split_axis=1, concat_axis=0, tiled=True),
        lax.all_to_all(own_keys, "seq", split_axis=1, concat_axis=0, tiled=True),
        lax.all_to_all(own_values, "seq", split_axis=1, concat_axis=0, tiled=True),
    )
    frame_rows = local_query.shape[0]
    half_feat = local_query.shape[1] // 2
    is_even = blk_index % 2 == 0

    def keep_give(whole):
        first = whole[:, :half_feat]
        second = whole[:, half_feat:]
        return (jnp.where(is_even, first, second), jnp.where(is_even, second, first))

    keep_q, give_q = keep_give(local_query)
    keep_k, give_k = keep_give(local_keys)
    keep_v, give_v = keep_give(local_values)
    got_q, got_k, got_v = partner((give_q, give_k, give_v), "blk", 0)

    def in_order(kept, got):
        return jnp.where(
            is_even, jnp.concatenate([kept, got], axis=0), jnp.concatenate([got, kept], axis=0)
        )

    pair_query = in_order(keep_q, got_q)
    held_keys = in_order(keep_k, got_k)
    held_values = in_order(keep_v, got_v)
    heads = half_feat // HDIM
    grouped = pair_query.reshape(2 * frame_rows, heads, HDIM)
    state = fold_keys(
        start_for(2 * frame_rows, heads), (held_keys, held_values), grouped, frame_rows
    )
    for bit in range(1, blk_count.bit_length() - 1):
        far_keys, far_values = partner((held_keys, held_values), "blk", bit)
        state = fold_keys(state, (far_keys, far_values), grouped, frame_rows)
        held_keys = jnp.concatenate([held_keys, far_keys], axis=0)
        held_values = jnp.concatenate([held_values, far_values], axis=0)
    paired_out = finish(state)
    mine_rows = jnp.where(is_even, paired_out[:frame_rows], paired_out[frame_rows:])
    their_rows = jnp.where(is_even, paired_out[frame_rows:], paired_out[:frame_rows])
    returned = partner(their_rows, "blk", 0)
    attended = jnp.where(
        is_even,
        jnp.concatenate([mine_rows, returned], axis=1),
        jnp.concatenate([returned, mine_rows], axis=1),
    )
    token_features = lax.all_to_all(attended, "seq", split_axis=0, concat_axis=1, tiled=True)
    velocity = jnp.dot(token_features, head_weight, preferred_element_type=jnp.float32)
    other = partner(velocity, "cfg", 0)
    is_cond = cfg_index == 0
    cond = jnp.where(is_cond, velocity, other)
    uncond = jnp.where(is_cond, other, velocity)
    guided = uncond + GUIDE * (cond - uncond)
    denoised = noisy_latents - NOISE_LEVEL * guided
    pixels = (
        denoised * jnp.tile(latent_std, 4)[None, :] + jnp.tile(latent_mean, 4)[None, :]
    ).astype(jnp.bfloat16)
    block_start = (blk_index * seq_count + seq_index) * tok_rows
    local_slot = patch_order - block_start
    selector = (jnp.arange(tok_rows, dtype=jnp.int32)[:, None] == local_slot[None, :]).astype(
        jnp.bfloat16
    )
    placed = jnp.dot(selector, pixels, preferred_element_type=jnp.float32).astype(jnp.bfloat16)
    grid_cols = COLS_DEV * blk_count
    strip_rows = tok_rows // grid_cols
    strip = placed.reshape(1, strip_rows, grid_cols * placed.shape[1])
    received = lax.all_to_all(strip, "blk", split_axis=2, concat_axis=0, tiled=True)
    frame_count = received.shape[0]
    tile = (
        received.reshape(frame_count, strip_rows, COLS_DEV, 2, 2, ZCH)
        .transpose(0, 1, 3, 2, 4, 5)
        .reshape(frame_count, 2 * strip_rows, 2 * COLS_DEV, ZCH)
    )
    half = frame_count // 2
    leading = jnp.zeros((2,) + tile.shape[1:], jnp.bfloat16)
    timeline = jnp.concatenate([leading, tile], axis=0)
    window = lax.dynamic_slice_in_dim(timeline, cfg_index * half, half + 2, 0)
    framed = padded(window, (("seq", 1), ("blk", 2)), 1)
    tile_rows = 2 * strip_rows
    tile_cols = 2 * COLS_DEV
    columns = []
    for step_t in range(3):
        for step_y in range(3):
            for step_x in range(3):
                columns.append(
                    framed[
                        step_t : step_t + half,
                        step_y : step_y + tile_rows,
                        step_x : step_x + tile_cols,
                        :,
                    ]
                )
    stacked = jnp.concatenate(columns, axis=3).reshape(half * tile_rows * tile_cols, 27 * ZCH)
    kernel = conv_weight.reshape(27 * ZCH, conv_weight.shape[4])
    output = jnp.dot(stacked, kernel, preferred_element_type=jnp.float32) + conv_bias[None, :]
    return output.reshape(half, tile_rows, tile_cols, conv_weight.shape[4]).astype(jnp.bfloat16)


def pack_kernel(order_ref, start_ref, q_ref, k_ref, v_ref, noisy_ref, send_ref, noise_ref):
    groups, rows, width = send_ref.shape
    feat = width // 3
    slot = order_ref[...] - start_ref[0]
    hit = lax.broadcasted_iota(jnp.int32, (rows, rows), 0) == slot
    selector = hit.astype(jnp.bfloat16)
    ordered = jnp.dot(selector, q_ref[...], preferred_element_type=jnp.float32)
    ordered = ordered.astype(jnp.bfloat16)
    for group in range(groups):
        cols = slice(group * feat, (group + 1) * feat)
        send_ref[group, :, :feat] = ordered[:, cols]
        send_ref[group, :, feat : 2 * feat] = k_ref[:, cols]
        send_ref[group, :, 2 * feat :] = v_ref[:, cols]
    noise_ref[...] = jnp.dot(
        hit.astype(jnp.float32),
        noisy_ref[...],
        preferred_element_type=jnp.float32,
        precision=lax.Precision.HIGHEST,
    )


def attend_kernel(place_ref, qkv_ref, weight_ref, noise_ref, pick_ref, out_ref, acc_ref):
    tokens, width = qkv_ref.shape
    feat = width // 3
    block = noise_ref.shape[0]
    scale = 1.0 / math.sqrt(HDIM)
    total_velocity = jnp.zeros(acc_ref.shape, jnp.float32)
    for head in range(feat // HDIM):
        low = head * HDIM
        query = qkv_ref[:, low : low + HDIM]
        key = qkv_ref[:, feat + low : feat + low + HDIM]
        value = qkv_ref[:, 2 * feat + low : 2 * feat + low + HDIM]
        scores = (
            lax.dot_general(
                query, key, (((1,), (1,)), ((), ())), preferred_element_type=jnp.float32
            )
            * scale
        )
        expo = jnp.exp(scores - jnp.max(scores, axis=1, keepdims=True))
        total = jnp.sum(expo, axis=1, keepdims=True)
        mixed = jnp.dot(
            expo.astype(jnp.bfloat16), value, preferred_element_type=jnp.float32
        )
        mixed = (mixed / total).astype(jnp.bfloat16)
        total_velocity = total_velocity + jnp.dot(
            mixed, weight_ref[low : low + HDIM, :], preferred_element_type=jnp.float32
        )
    is_cond = place_ref[1] == 0
    factor = jnp.where(is_cond, -NOISE_LEVEL * GUIDE, -NOISE_LEVEL * (1.0 - GUIDE))
    acc_ref[...] = total_velocity * factor
    rows = pl.ds(pl.multiple_of(place_ref[0] * block, 8), block)
    acc_ref[rows, :] = acc_ref[rows, :] + noise_ref[...] * jnp.where(is_cond, 1.0, 0.0)
    share = acc_ref[...].astype(jnp.bfloat16)
    both = jnp.concatenate([share[: tokens // 2], share[tokens // 2 :]], axis=1)
    placed = jnp.dot(pick_ref[...], both, preferred_element_type=jnp.float32)
    placed = placed.astype(jnp.bfloat16)
    rows_each = out_ref.shape[2]
    for group in range(out_ref.shape[0]):
        piece = placed[group * rows_each : (group + 1) * rows_each]
        for core in range(out_ref.shape[1]):
            out_ref[group, core] = piece


def conv_kernel(
    place_ref, got_ref, std_ref, mean_ref, mesh_ref, weight_ref, bias_ref, order_ref, out_ref, big_ref
):
    frames_out, tile_rows, tile_cols, channels = out_ref.shape
    wide = tile_cols // 2
    high = tile_rows // 2
    shares, rows, lanes = got_ref.shape
    summed = got_ref[0].astype(jnp.float32)
    for share in range(1, shares):
        summed = summed + got_ref[share].astype(jnp.float32)
    span = wide + 2
    tall = high + 2
    row = lax.broadcasted_iota(jnp.int32, (rows, lanes), 0)
    col_at = place_ref[0] * wide - 1 + row % span
    row_at = place_ref[1] * high - 1 + row // span % tall
    inside = (
        (col_at >= 0) & (col_at < place_ref[3]) & (row_at >= 0) & (row_at < place_ref[4])
    )
    pixels = jnp.where(inside, summed * std_ref[...] + mean_ref[...], 0.0)
    half = lanes // 2
    flat = jnp.concatenate([pixels[:, :half], pixels[:, half:]], axis=0)
    count = 2 * rows
    moved = pltpu.roll(flat, count - 1, 0)
    pairs = jnp.concatenate([flat, moved], axis=1).astype(jnp.bfloat16)
    wanted = mesh_ref[:, 0:1] + place_ref[2] * (frames_out * tall * span)
    hits = (lax.broadcasted_iota(jnp.int32, (mesh_ref.shape[0], count), 1) == wanted).astype(
        jnp.bfloat16
    )
    pieces = jnp.dot(hits, pairs, preferred_element_type=jnp.float32).astype(jnp.bfloat16)
    part = frames_out * high * wide
    part = (part + 15) // 16 * 16
    big_ref[...] = jnp.zeros(big_ref.shape, big_ref.dtype)
    results = []
    for down in range(2):
        for right in range(2):
            which = down * 2 + right
            for step_t in range(3):
                for step_y in range(3):
                    for step_x in range(3):
                        y = 1 - down + step_y
                        x = 1 - right + step_x
                        at = (step_t * 2 + y // 2) * 8 + (x // 2) * 4 + (y % 2) * 2 + x % 2
                        big_ref[which, at * ZCH : (at + 1) * ZCH, :] = weight_ref[
                            (step_t * 3 + step_y) * 3 + step_x
                        ]
            columns = []
            for step_t in range(3):
                for near in range(2):
                    at = (step_t * 3 + down + near) * 2 + right
                    columns.append(pieces[at * part : (at + 1) * part])
            stacked = jnp.concatenate(columns, axis=1)
            result = jnp.dot(stacked, big_ref[which], preferred_element_type=jnp.float32)
            results.append((result + bias_ref[...]).astype(jnp.bfloat16))
    together = jnp.concatenate(results, axis=0)
    final = jnp.dot(order_ref[...], together, preferred_element_type=jnp.float32)
    final = final.astype(jnp.bfloat16)
    for frame in range(frames_out):
        for y in range(tile_rows):
            at = (frame * tile_rows + y) * 8
            out_ref[frame, y] = final[at : at + tile_cols]


def tile_rows_of(seq_count, blk_count, frames, high, wide):
    grid_rows = seq_count * high
    grid_cols = blk_count * wide
    table = np.full((blk_count, seq_count, frames // 2, high + 2, wide + 2), -1, np.int32)
    for blk in range(blk_count):
        for seq in range(seq_count):
            for frame in range(frames // 2):
                for i in range(high + 2):
                    for w in range(wide + 2):
                        y = seq * high - 1 + i
                        x = blk * wide - 1 + w
                        if 0 <= y < grid_rows and 0 <= x < grid_cols:
                            table[blk, seq, frame, i, w] = (frame * grid_rows + y) * grid_cols + x
    return table.reshape(-1)


def window_rows(frames_out, high, wide):
    part = (frames_out * high * wide + 15) // 16 * 16
    table = np.full((3, 3, 2, part), -100000, np.int32)
    for step_t in range(3):
        for near in range(3):
            for right in range(2):
                for frame in range(frames_out):
                    for i in range(high):
                        for w in range(wide):
                            source = frame - 2 + step_t
                            at = (source * (high + 2) + i + near) * (wide + 2) + w + right
                            if source < 0:
                                at = (source * (high + 2) + i + near) * (wide + 2) + w + right
                            table[step_t, near, right, (frame * high + i) * wide + w] = at
    return table.reshape(-1, 1)


def output_order(frames_out, high, wide):
    part = (frames_out * high * wide + 15) // 16 * 16
    table = np.zeros((frames_out * 2 * high * 8, 4 * part), np.float32)
    for frame in range(frames_out):
        for y in range(2 * high):
            for x in range(2 * wide):
                which = (y % 2) * 2 + x % 2
                source = which * part + (frame * high + y // 2) * wide + x // 2
                table[(frame * 2 * high + y) * 8 + x, source] = 1.0
    return table


def exchange(packed):
    return lax.all_to_all(packed, ("blk", "seq"), split_axis=0, concat_axis=0, tiled=True)


def by_heads(
    queries,
    key_states,
    value_states,
    noisy_latents,
    patch_order,
    head_weight,
    latent_std,
    latent_mean,
    conv_weight,
    conv_bias,
):
    seq_count = lax.axis_size("seq")
    blk_count = lax.axis_size("blk")
    cfg_count = lax.axis_size("cfg")
    seq_index = lax.axis_index("seq")
    blk_index = lax.axis_index("blk")
    cfg_index = lax.axis_index("cfg")
    groups = seq_count * blk_count
    block = queries.shape[1]
    tokens = groups * block
    feat = queries.shape[2] // groups
    patch = noisy_latents.shape[1]
    channels = conv_weight.shape[4]
    own = (blk_index * seq_count + seq_index).astype(jnp.int32)
    frames = blk_count
    grid_cols = COLS_DEV * blk_count
    high = block // grid_cols
    wide = COLS_DEV
    vmem = pl.BlockSpec(memory_space=pltpu.VMEM)
    smem = pl.BlockSpec(memory_space=pltpu.SMEM)
    packed, noise = pl.pallas_call(
        pack_kernel,
        out_shape=(
            jax.ShapeDtypeStruct((groups, block, 3 * feat), jnp.bfloat16),
            jax.ShapeDtypeStruct((block, patch), jnp.float32),
        ),
        in_specs=[vmem, smem, vmem, vmem, vmem, vmem],
        out_specs=(vmem, vmem),
    )(
        patch_order[None, :],
        (own * block)[None],
        queries[0],
        key_states[0],
        value_states[0],
        noisy_latents,
    )
    received = exchange(packed).reshape(tokens, 3 * feat)
    weight = lax.dynamic_slice_in_dim(head_weight, own * feat, feat, 0)
    pick = (
        np.arange(tokens // 2)[None, :]
        == tile_rows_of(seq_count, blk_count, frames, high, wide)[:, None]
    )
    tile = frames // 2 * (high + 2) * (wide + 2)
    shares = pl.pallas_call(
        attend_kernel,
        out_shape=jax.ShapeDtypeStruct((groups, cfg_count, tile, 2 * patch), jnp.bfloat16),
        in_specs=[smem, vmem, vmem, vmem, vmem],
        out_specs=vmem,
        scratch_shapes=[pltpu.VMEM((tokens, patch), jnp.float32)],
    )(
        jnp.stack([own, cfg_index.astype(jnp.int32)]),
        received,
        weight,
        noise,
        jnp.asarray(pick, jnp.bfloat16),
    )
    got = lax.all_to_all(
        shares.reshape(groups * cfg_count, tile, 2 * patch),
        ("blk", "seq", "cfg"),
        split_axis=0,
        concat_axis=0,
        tiled=True,
    )
    place = jnp.stack(
        [blk_index, seq_index, cfg_index, jnp.int32(grid_cols), jnp.int32(seq_count * high)]
    ).astype(jnp.int32)
    frames_out = frames // cfg_count
    return pl.pallas_call(
        conv_kernel,
        out_shape=jax.ShapeDtypeStruct((frames_out, 2 * high, 2 * wide, channels), jnp.bfloat16),
        in_specs=[smem] + [vmem] * 7,
        out_specs=vmem,
        scratch_shapes=[pltpu.VMEM((4, 48 * ZCH, channels), jnp.bfloat16)],
    )(
        place,
        got,
        jnp.tile(latent_std, 2 * patch // ZCH)[None, :],
        jnp.tile(latent_mean, 2 * patch // ZCH)[None, :],
        jnp.asarray(window_rows(frames_out, high, wide)),
        conv_weight.reshape(27, ZCH, channels),
        conv_bias[None, :],
        jnp.asarray(output_order(frames_out, high, wide), jnp.bfloat16),
    )


def chosen(*arrays):
    groups = lax.axis_size("seq") * lax.axis_size("blk")
    heads = arrays[0].shape[2] // HDIM
    if heads % groups == 0:
        return by_heads(*arrays)
    return local(*arrays)


def solution(mesh):
    in_specs = (
        P("cfg", ("prompt", "blk", "seq"), None),
        P("cfg", ("prompt", "blk", "seq"), None),
        P("cfg", ("prompt", "blk", "seq"), None),
        P(("prompt", "blk", "seq"), None),
        P(("prompt", "blk", "seq")),
        P(),
        P(),
        P(),
        P(),
        P(),
    )
    out_specs = P(("prompt", "cfg"), "seq", "blk", None)
    return jax.shard_map(chosen, mesh=mesh, in_specs=in_specs, out_specs=out_specs, check_vma=False)
```

```python
import math

import jax
import jax.numpy as jnp
import numpy as np
from jax import lax
from jax.experimental import pallas as pl
from jax.experimental.pallas import tpu as pltpu
from jax.sharding import PartitionSpec as P

HDIM = 128
ZCH = 16
COLS_DEV = 3


GUIDE = 5.0
NOISE_LEVEL = 0.5


def partner(array, axis, apart):
    return lax.ppermute(array, axis, [(i, i ^ 1 << apart) for i in range(lax.axis_size(axis))])


def padded(array, sides, width):
    for axis, dim in sides:
        devices, length = (lax.axis_size(axis), array.shape[dim])
        up = [(i, (i + 1) % devices) for i in range(devices - 1)]
        down = [(j, i) for i, j in up]
        last = lax.slice_in_dim(array, length - width, length, axis=dim)
        first = lax.slice_in_dim(array, 0, width, axis=dim)
        before = lax.ppermute(last, axis, up)
        after = lax.ppermute(first, axis, down)
        array = jnp.concatenate([before, array, after], axis=dim)
    return array


def fold_keys(carry, piece, grouped, block):
    keys_piece, values_piece = piece
    heads = grouped.shape[1]
    count = keys_piece.shape[0] // block
    key_blocks = keys_piece.reshape(count, block, heads, HDIM)
    value_blocks = values_piece.reshape(count, block, heads, HDIM)
    scale = 1.0 / math.sqrt(HDIM)

    def one_block(state, pair):
        top, total, acc = state
        key_block, value_block = pair
        scores = (
            jnp.einsum("qhd,khd->hqk", grouped, key_block, preferred_element_type=jnp.float32)
            * scale
        )
        new_top = jnp.maximum(top, jnp.max(scores, axis=2))
        expo = jnp.exp(scores - new_top[:, :, None])
        factor = jnp.exp(top - new_top)
        total = total * factor + jnp.sum(expo, axis=2)
        weights = expo.astype(jnp.bfloat16)
        update = jnp.einsum(
            "hqk,khd->qhd", weights, value_block, preferred_element_type=jnp.float32
        )
        acc = acc * factor.T[:, :, None] + update
        return ((new_top, total, acc), None)

    state, unused = lax.scan(one_block, carry, (key_blocks, value_blocks))
    return state


def start_for(rows, heads):
    return (
        jnp.full((heads, rows), -1e30, jnp.float32),
        jnp.zeros((heads, rows), jnp.float32),
        jnp.zeros((rows, heads, HDIM), jnp.float32),
    )


def finish(state):
    top, total, acc = state
    rows = acc.shape[0]
    return (acc / total.T[:, :, None]).astype(jnp.bfloat16).reshape(rows, acc.shape[1] * HDIM)


def local(
    queries,
    key_states,
    value_states,
    noisy_latents,
    patch_order,
    head_weight,
    latent_std,
    latent_mean,
    conv_weight,
    conv_bias,
):
    seq_count = lax.axis_size("seq")
    blk_count = lax.axis_size("blk")
    seq_index = lax.axis_index("seq")
    blk_index = lax.axis_index("blk")
    cfg_index = lax.axis_index("cfg")
    tok_rows = queries.shape[1]
    own_query = queries[0]
    own_keys = key_states[0]
    own_values = value_states[0]
    local_query, local_keys, local_values = (
        lax.all_to_all(own_query, "seq", split_axis=1, concat_axis=0, tiled=True),
        lax.all_to_all(own_keys, "seq", split_axis=1, concat_axis=0, tiled=True),
        lax.all_to_all(own_values, "seq", split_axis=1, concat_axis=0, tiled=True),
    )
    frame_rows = local_query.shape[0]
    half_feat = local_query.shape[1] // 2
    is_even = blk_index % 2 == 0

    def keep_give(whole):
        first = whole[:, :half_feat]
        second = whole[:, half_feat:]
        return (jnp.where(is_even, first, second), jnp.where(is_even, second, first))

    keep_q, give_q = keep_give(local_query)
    keep_k, give_k = keep_give(local_keys)
    keep_v, give_v = keep_give(local_values)
    got_q, got_k, got_v = partner((give_q, give_k, give_v), "blk", 0)

    def in_order(kept, got):
        return jnp.where(
            is_even, jnp.concatenate([kept, got], axis=0), jnp.concatenate([got, kept], axis=0)
        )

    pair_query = in_order(keep_q, got_q)
    held_keys = in_order(keep_k, got_k)
    held_values = in_order(keep_v, got_v)
    heads = half_feat // HDIM
    grouped = pair_query.reshape(2 * frame_rows, heads, HDIM)
    state = fold_keys(
        start_for(2 * frame_rows, heads), (held_keys, held_values), grouped, frame_rows
    )
    for bit in range(1, blk_count.bit_length() - 1):
        far_keys, far_values = partner((held_keys, held_values), "blk", bit)
        state = fold_keys(state, (far_keys, far_values), grouped, frame_rows)
        held_keys = jnp.concatenate([held_keys, far_keys], axis=0)
        held_values = jnp.concatenate([held_values, far_values], axis=0)
    paired_out = finish(state)
    mine_rows = jnp.where(is_even, paired_out[:frame_rows], paired_out[frame_rows:])
    their_rows = jnp.where(is_even, paired_out[frame_rows:], paired_out[:frame_rows])
    returned = partner(their_rows, "blk", 0)
    attended = jnp.where(
        is_even,
        jnp.concatenate([mine_rows, returned], axis=1),
        jnp.concatenate([returned, mine_rows], axis=1),
    )
    token_features = lax.all_to_all(attended, "seq", split_axis=0, concat_axis=1, tiled=True)
    velocity = jnp.dot(token_features, head_weight, preferred_element_type=jnp.float32)
    other = partner(velocity, "cfg", 0)
    is_cond = cfg_index == 0
    cond = jnp.where(is_cond, velocity, other)
    uncond = jnp.where(is_cond, other, velocity)
    guided = uncond + GUIDE * (cond - uncond)
    denoised = noisy_latents - NOISE_LEVEL * guided
    pixels = (
        denoised * jnp.tile(latent_std, 4)[None, :] + jnp.tile(latent_mean, 4)[None, :]
    ).astype(jnp.bfloat16)
    block_start = (blk_index * seq_count + seq_index) * tok_rows
    local_slot = patch_order - block_start
    selector = (jnp.arange(tok_rows, dtype=jnp.int32)[:, None] == local_slot[None, :]).astype(
        jnp.bfloat16
    )
    placed = jnp.dot(selector, pixels, preferred_element_type=jnp.float32).astype(jnp.bfloat16)
    grid_cols = COLS_DEV * blk_count
    strip_rows = tok_rows // grid_cols
    strip = placed.reshape(1, strip_rows, grid_cols * placed.shape[1])
    received = lax.all_to_all(strip, "blk", split_axis=2, concat_axis=0, tiled=True)
    frame_count = received.shape[0]
    tile = (
        received.reshape(frame_count, strip_rows, COLS_DEV, 2, 2, ZCH)
        .transpose(0, 1, 3, 2, 4, 5)
        .reshape(frame_count, 2 * strip_rows, 2 * COLS_DEV, ZCH)
    )
    half = frame_count // 2
    leading = jnp.zeros((2,) + tile.shape[1:], jnp.bfloat16)
    timeline = jnp.concatenate([leading, tile], axis=0)
    window = lax.dynamic_slice_in_dim(timeline, cfg_index * half, half + 2, 0)
    framed = padded(window, (("seq", 1), ("blk", 2)), 1)
    tile_rows = 2 * strip_rows
    tile_cols = 2 * COLS_DEV
    columns = []
    for step_t in range(3):
        for step_y in range(3):
            for step_x in range(3):
                columns.append(
                    framed[
                        step_t : step_t + half,
                        step_y : step_y + tile_rows,
                        step_x : step_x + tile_cols,
                        :,
                    ]
                )
    stacked = jnp.concatenate(columns, axis=3).reshape(half * tile_rows * tile_cols, 27 * ZCH)
    kernel = conv_weight.reshape(27 * ZCH, conv_weight.shape[4])
    output = jnp.dot(stacked, kernel, preferred_element_type=jnp.float32) + conv_bias[None, :]
    return output.reshape(half, tile_rows, tile_cols, conv_weight.shape[4]).astype(jnp.bfloat16)


def pack_kernel(order_ref, start_ref, q_ref, k_ref, v_ref, head_ref, noisy_ref, send_ref, noise_ref):
    groups, rows, width = send_ref.shape
    patch = noise_ref.shape[1]
    feat = width * HDIM // (2 * HDIM + patch)
    slot = order_ref[...] - start_ref[0]
    hit = lax.broadcasted_iota(jnp.int32, (rows, rows), 0) == slot
    selector = hit.astype(jnp.bfloat16)
    ordered = jnp.dot(selector, q_ref[...], preferred_element_type=jnp.float32)
    ordered = ordered.astype(jnp.bfloat16)
    for group in range(groups):
        cols = slice(group * feat, (group + 1) * feat)
        send_ref[group, :, :feat] = ordered[:, cols]
        send_ref[group, :, feat : 2 * feat] = k_ref[:, cols]
        for head in range(0, feat // HDIM, 2):
            low = group * feat + head * HDIM
            both = [
                lax.dot_general(
                    v_ref[:, at : at + HDIM],
                    head_ref[:, at : at + HDIM],
                    (((1,), (1,)), ((), ())),
                    preferred_element_type=jnp.float32,
                )
                for at in (low, low + HDIM)
            ]
            at = 2 * feat + head * patch
            send_ref[group, :, at : at + 2 * patch] = jnp.concatenate(both, axis=1).astype(
                jnp.bfloat16
            )
    noise_ref[...] = jnp.dot(
        hit.astype(jnp.float32),
        noisy_ref[...],
        preferred_element_type=jnp.float32,
        precision=lax.Precision.HIGHEST,
    )


def attend_kernel(place_ref, qkv_ref, noise_ref, pick_ref, out_ref, acc_ref):
    tokens, width = qkv_ref.shape
    patch = acc_ref.shape[1]
    feat = width * HDIM // (2 * HDIM + patch)
    block = noise_ref.shape[0]
    scale = 1.0 / math.sqrt(HDIM)
    wide_velocity = jnp.zeros((tokens, 2 * patch), jnp.float32)
    lane = lax.broadcasted_iota(jnp.int32, (tokens, 2 * patch), 1)
    for head in range(feat // HDIM):
        low = head * HDIM
        query = qkv_ref[:, low : low + HDIM]
        key = qkv_ref[:, feat + low : feat + low + HDIM]
        pair = 2 * feat + head // 2 * 2 * patch
        value = qkv_ref[:, pair : pair + 2 * patch]
        scores = (
            lax.dot_general(
                query, key, (((1,), (1,)), ((), ())), preferred_element_type=jnp.float32
            )
            * scale
        )
        expo = jnp.exp(scores - jnp.max(scores, axis=1, keepdims=True))
        total = jnp.sum(expo, axis=1, keepdims=True)
        mixed = jnp.dot(
            expo.astype(jnp.bfloat16), value, preferred_element_type=jnp.float32
        )
        mine = lane // patch == head % 2
        wide_velocity = wide_velocity + jnp.where(mine, mixed / total, 0.0)
    is_cond = place_ref[1] == 0
    factor = jnp.where(is_cond, -NOISE_LEVEL * GUIDE, -NOISE_LEVEL * (1.0 - GUIDE))
    acc_ref[...] = (wide_velocity[:, :patch] + wide_velocity[:, patch:]) * factor
    rows = pl.ds(pl.multiple_of(place_ref[0] * block, 8), block)
    acc_ref[rows, :] = acc_ref[rows, :] + noise_ref[...] * jnp.where(is_cond, 1.0, 0.0)
    share = acc_ref[...].astype(jnp.bfloat16)
    both = jnp.concatenate([share[: tokens // 2], share[tokens // 2 :]], axis=1)
    placed = jnp.dot(pick_ref[...], both, preferred_element_type=jnp.float32)
    placed = placed.astype(jnp.bfloat16)
    rows_each = out_ref.shape[2]
    for group in range(out_ref.shape[0]):
        piece = placed[group * rows_each : (group + 1) * rows_each]
        for core in range(out_ref.shape[1]):
            out_ref[group, core] = piece


def conv_kernel(
    place_ref,
    got_ref,
    std_ref,
    mean_ref,
    mesh_ref,
    weight_ref,
    bias_ref,
    order_ref,
    out_ref,
    big_ref,
):
    big_ref[...] = jnp.zeros(big_ref.shape, big_ref.dtype)
    frames_out, tile_cols, tile_rows, channels = out_ref.shape
    wide = tile_cols // 2
    high = tile_rows // 2
    shares, rows, lanes = got_ref.shape
    for down in range(2):
        for right in range(2):
            which = down * 2 + right
            for step_t in range(3):
                for step_y in range(3):
                    for step_x in range(3):
                        y = 1 - down + step_y
                        x = 1 - right + step_x
                        at = (step_t * 2 + y // 2) * 8 + (x // 2) * 4 + (y % 2) * 2 + x % 2
                        big_ref[which, at * ZCH : (at + 1) * ZCH, :] = weight_ref[
                            (step_t * 3 + step_y) * 3 + step_x
                        ]
    summed = got_ref[0].astype(jnp.float32)
    for share in range(1, shares):
        summed = summed + got_ref[share].astype(jnp.float32)
    span = wide + 2
    tall = high + 2
    row = lax.broadcasted_iota(jnp.int32, (rows, lanes), 0)
    col_at = place_ref[0] * wide - 1 + row % span
    row_at = place_ref[1] * high - 1 + row // span % tall
    inside = (
        (col_at >= 0) & (col_at < place_ref[3]) & (row_at >= 0) & (row_at < place_ref[4])
    )
    pixels = jnp.where(inside, summed * std_ref[...] + mean_ref[...], 0.0)
    half = lanes // 2
    flat = jnp.concatenate([pixels[:, :half], pixels[:, half:]], axis=0)
    count = 2 * rows
    moved = pltpu.roll(flat, count - 1, 0)
    pairs = jnp.concatenate([flat, moved], axis=1).astype(jnp.bfloat16)
    wanted = mesh_ref[:, 0:1] + place_ref[2] * (frames_out * tall * span)
    hits = (lax.broadcasted_iota(jnp.int32, (mesh_ref.shape[0], count), 1) == wanted).astype(
        jnp.bfloat16
    )
    pieces = jnp.dot(hits, pairs, preferred_element_type=jnp.float32).astype(jnp.bfloat16)
    part = frames_out * high * wide
    part = (part + 15) // 16 * 16
    results = []
    for down in range(2):
        for right in range(2):
            which = down * 2 + right
            columns = []
            for step_t in range(3):
                for near in range(2):
                    at = (step_t * 3 + down + near) * 2 + right
                    columns.append(pieces[at * part : (at + 1) * part])
            stacked = jnp.concatenate(columns, axis=1)
            result = jnp.dot(stacked, big_ref[which], preferred_element_type=jnp.float32)
            results.append((result + bias_ref[...]).astype(jnp.bfloat16))
    together = jnp.concatenate(results, axis=0)
    final = jnp.dot(order_ref[...], together, preferred_element_type=jnp.float32)
    final = final.astype(jnp.bfloat16)
    for frame in range(frames_out):
        for x in range(tile_cols):
            at = (frame * tile_cols + x) * 8
            out_ref[frame, x] = final[at : at + tile_rows]


def tile_rows_of(seq_count, blk_count, frames, high, wide):
    grid_rows = seq_count * high
    grid_cols = blk_count * wide
    table = np.full((blk_count, seq_count, frames // 2, high + 2, wide + 2), -1, np.int32)
    for blk in range(blk_count):
        for seq in range(seq_count):
            for frame in range(frames // 2):
                for i in range(high + 2):
                    for w in range(wide + 2):
                        y = seq * high - 1 + i
                        x = blk * wide - 1 + w
                        if 0 <= y < grid_rows and 0 <= x < grid_cols:
                            table[blk, seq, frame, i, w] = (frame * grid_rows + y) * grid_cols + x
    return table.reshape(-1)


def window_rows(frames_out, high, wide):
    part = (frames_out * high * wide + 15) // 16 * 16
    table = np.full((3, 3, 2, part), -100000, np.int32)
    for step_t in range(3):
        for near in range(3):
            for right in range(2):
                for frame in range(frames_out):
                    for i in range(high):
                        for w in range(wide):
                            source = frame - 2 + step_t
                            at = (source * (high + 2) + i + near) * (wide + 2) + w + right
                            if source < 0:
                                at = (source * (high + 2) + i + near) * (wide + 2) + w + right
                            table[step_t, near, right, (frame * high + i) * wide + w] = at
    return table.reshape(-1, 1)


def output_order(frames_out, high, wide):
    part = (frames_out * high * wide + 15) // 16 * 16
    table = np.zeros((frames_out * 2 * wide * 8, 4 * part), np.float32)
    for frame in range(frames_out):
        for y in range(2 * high):
            for x in range(2 * wide):
                which = (y % 2) * 2 + x % 2
                source = which * part + (frame * high + y // 2) * wide + x // 2
                table[(frame * 2 * wide + x) * 8 + y, source] = 1.0
    return table


def exchange(packed):
    return lax.all_to_all(packed, ("blk", "seq"), split_axis=0, concat_axis=0, tiled=True)


def by_heads(
    queries,
    key_states,
    value_states,
    noisy_latents,
    patch_order,
    head_weight,
    latent_std,
    latent_mean,
    conv_weight,
    conv_bias,
):
    seq_count = lax.axis_size("seq")
    blk_count = lax.axis_size("blk")
    cfg_count = lax.axis_size("cfg")
    seq_index = lax.axis_index("seq")
    blk_index = lax.axis_index("blk")
    cfg_index = lax.axis_index("cfg")
    groups = seq_count * blk_count
    block = queries.shape[1]
    tokens = groups * block
    feat = queries.shape[2] // groups
    patch = noisy_latents.shape[1]
    width = 2 * feat + feat // HDIM * patch
    channels = conv_weight.shape[4]
    own = (blk_index * seq_count + seq_index).astype(jnp.int32)
    frames = blk_count
    grid_cols = COLS_DEV * blk_count
    high = block // grid_cols
    wide = COLS_DEV
    vmem = pl.BlockSpec(memory_space=pltpu.VMEM)
    smem = pl.BlockSpec(memory_space=pltpu.SMEM)
    packed, noise = pl.pallas_call(
        pack_kernel,
        out_shape=(
            pltpu.VMEM((groups, block, width), jnp.bfloat16),
            pltpu.VMEM((block, patch), jnp.float32),
        ),
        in_specs=[vmem, smem, vmem, vmem, vmem, vmem, vmem],
        out_specs=(vmem, vmem),
    )(
        patch_order[None, :],
        (own * block)[None],
        queries[0],
        key_states[0],
        value_states[0],
        head_weight.T,
        noisy_latents,
    )
    received = pltpu.with_memory_space_constraint(
        exchange(packed).reshape(tokens, width), pltpu.VMEM
    )
    pick = (
        np.arange(tokens // 2)[None, :]
        == tile_rows_of(seq_count, blk_count, frames, high, wide)[:, None]
    )
    tile = frames // 2 * (high + 2) * (wide + 2)
    shares = pl.pallas_call(
        attend_kernel,
        out_shape=pltpu.VMEM((groups, cfg_count, tile, 2 * patch), jnp.bfloat16),
        in_specs=[smem] + [vmem] * 3,
        out_specs=vmem,
        scratch_shapes=[
            pltpu.VMEM((tokens, patch), jnp.float32),
        ],
    )(
        jnp.stack([own, cfg_index.astype(jnp.int32)]),
        received,
        pltpu.with_memory_space_constraint(noise, pltpu.VMEM),
        jnp.asarray(pick, jnp.bfloat16),
    )
    got = lax.all_to_all(
        shares.reshape(groups * cfg_count, tile, 2 * patch),
        ("blk", "seq", "cfg"),
        split_axis=0,
        concat_axis=0,
        tiled=True,
    )
    place = jnp.stack(
        [blk_index, seq_index, cfg_index, jnp.int32(grid_cols), jnp.int32(seq_count * high)]
    ).astype(jnp.int32)
    frames_out = frames // cfg_count
    features = pl.pallas_call(
        conv_kernel,
        out_shape=jax.ShapeDtypeStruct((frames_out, 2 * wide, 2 * high, channels), jnp.bfloat16),
        in_specs=[smem] + [vmem] * 7,
        out_specs=vmem,
        scratch_shapes=[
            pltpu.VMEM((4, 48 * ZCH, channels), jnp.bfloat16),
        ],
    )(
        place,
        pltpu.with_memory_space_constraint(got, pltpu.VMEM),
        jnp.tile(latent_std, 2 * patch // ZCH)[None, :],
        jnp.tile(latent_mean, 2 * patch // ZCH)[None, :],
        jnp.asarray(window_rows(frames_out, high, wide)),
        conv_weight.reshape(27, ZCH, channels),
        conv_bias[None, :],
        jnp.asarray(output_order(frames_out, high, wide), jnp.bfloat16),
    )
    return features.transpose(0, 2, 1, 3)


def chosen(*arrays):
    groups = lax.axis_size("seq") * lax.axis_size("blk")
    heads = arrays[0].shape[2] // HDIM
    if heads % (2 * groups) == 0:
        return by_heads(*arrays)
    return local(*arrays)


def solution(mesh):
    in_specs = (
        P("cfg", ("prompt", "blk", "seq"), None),
        P("cfg", ("prompt", "blk", "seq"), None),
        P("cfg", ("prompt", "blk", "seq"), None),
        P(("prompt", "blk", "seq"), None),
        P(("prompt", "blk", "seq")),
        P(),
        P(),
        P(),
        P(),
        P(),
    )
    out_specs = P(("prompt", "cfg"), "seq", "blk", None)
    return jax.shard_map(chosen, mesh=mesh, in_specs=in_specs, out_specs=out_specs, check_vma=False)
```

```python
import math

import jax
import jax.numpy as jnp
import numpy as np
from jax import lax
from jax.experimental import pallas as pl
from jax.experimental.pallas import tpu as pltpu
from jax.sharding import PartitionSpec as P

HDIM = 128
ZCH = 16
COLS_DEV = 3


GUIDE = 5.0
NOISE_LEVEL = 0.5


def partner(array, axis, apart):
    return lax.ppermute(array, axis, [(i, i ^ 1 << apart) for i in range(lax.axis_size(axis))])


def padded(array, sides, width):
    for axis, dim in sides:
        devices, length = (lax.axis_size(axis), array.shape[dim])
        up = [(i, (i + 1) % devices) for i in range(devices - 1)]
        down = [(j, i) for i, j in up]
        last = lax.slice_in_dim(array, length - width, length, axis=dim)
        first = lax.slice_in_dim(array, 0, width, axis=dim)
        before = lax.ppermute(last, axis, up)
        after = lax.ppermute(first, axis, down)
        array = jnp.concatenate([before, array, after], axis=dim)
    return array


def fold_keys(carry, piece, grouped, block):
    keys_piece, values_piece = piece
    heads = grouped.shape[1]
    count = keys_piece.shape[0] // block
    key_blocks = keys_piece.reshape(count, block, heads, HDIM)
    value_blocks = values_piece.reshape(count, block, heads, HDIM)
    scale = 1.0 / math.sqrt(HDIM)

    def one_block(state, pair):
        top, total, acc = state
        key_block, value_block = pair
        scores = (
            jnp.einsum("qhd,khd->hqk", grouped, key_block, preferred_element_type=jnp.float32)
            * scale
        )
        new_top = jnp.maximum(top, jnp.max(scores, axis=2))
        expo = jnp.exp(scores - new_top[:, :, None])
        factor = jnp.exp(top - new_top)
        total = total * factor + jnp.sum(expo, axis=2)
        weights = expo.astype(jnp.bfloat16)
        update = jnp.einsum(
            "hqk,khd->qhd", weights, value_block, preferred_element_type=jnp.float32
        )
        acc = acc * factor.T[:, :, None] + update
        return ((new_top, total, acc), None)

    state, unused = lax.scan(one_block, carry, (key_blocks, value_blocks))
    return state


def start_for(rows, heads):
    return (
        jnp.full((heads, rows), -1e30, jnp.float32),
        jnp.zeros((heads, rows), jnp.float32),
        jnp.zeros((rows, heads, HDIM), jnp.float32),
    )


def finish(state):
    top, total, acc = state
    rows = acc.shape[0]
    return (acc / total.T[:, :, None]).astype(jnp.bfloat16).reshape(rows, acc.shape[1] * HDIM)


def local(
    queries,
    key_states,
    value_states,
    noisy_latents,
    patch_order,
    head_weight,
    latent_std,
    latent_mean,
    conv_weight,
    conv_bias,
):
    seq_count = lax.axis_size("seq")
    blk_count = lax.axis_size("blk")
    seq_index = lax.axis_index("seq")
    blk_index = lax.axis_index("blk")
    cfg_index = lax.axis_index("cfg")
    tok_rows = queries.shape[1]
    own_query = queries[0]
    own_keys = key_states[0]
    own_values = value_states[0]
    local_query, local_keys, local_values = (
        lax.all_to_all(own_query, "seq", split_axis=1, concat_axis=0, tiled=True),
        lax.all_to_all(own_keys, "seq", split_axis=1, concat_axis=0, tiled=True),
        lax.all_to_all(own_values, "seq", split_axis=1, concat_axis=0, tiled=True),
    )
    frame_rows = local_query.shape[0]
    half_feat = local_query.shape[1] // 2
    is_even = blk_index % 2 == 0

    def keep_give(whole):
        first = whole[:, :half_feat]
        second = whole[:, half_feat:]
        return (jnp.where(is_even, first, second), jnp.where(is_even, second, first))

    keep_q, give_q = keep_give(local_query)
    keep_k, give_k = keep_give(local_keys)
    keep_v, give_v = keep_give(local_values)
    got_q, got_k, got_v = partner((give_q, give_k, give_v), "blk", 0)

    def in_order(kept, got):
        return jnp.where(
            is_even, jnp.concatenate([kept, got], axis=0), jnp.concatenate([got, kept], axis=0)
        )

    pair_query = in_order(keep_q, got_q)
    held_keys = in_order(keep_k, got_k)
    held_values = in_order(keep_v, got_v)
    heads = half_feat // HDIM
    grouped = pair_query.reshape(2 * frame_rows, heads, HDIM)
    state = fold_keys(
        start_for(2 * frame_rows, heads), (held_keys, held_values), grouped, frame_rows
    )
    for bit in range(1, blk_count.bit_length() - 1):
        far_keys, far_values = partner((held_keys, held_values), "blk", bit)
        state = fold_keys(state, (far_keys, far_values), grouped, frame_rows)
        held_keys = jnp.concatenate([held_keys, far_keys], axis=0)
        held_values = jnp.concatenate([held_values, far_values], axis=0)
    paired_out = finish(state)
    mine_rows = jnp.where(is_even, paired_out[:frame_rows], paired_out[frame_rows:])
    their_rows = jnp.where(is_even, paired_out[frame_rows:], paired_out[:frame_rows])
    returned = partner(their_rows, "blk", 0)
    attended = jnp.where(
        is_even,
        jnp.concatenate([mine_rows, returned], axis=1),
        jnp.concatenate([returned, mine_rows], axis=1),
    )
    token_features = lax.all_to_all(attended, "seq", split_axis=0, concat_axis=1, tiled=True)
    velocity = jnp.dot(token_features, head_weight, preferred_element_type=jnp.float32)
    other = partner(velocity, "cfg", 0)
    is_cond = cfg_index == 0
    cond = jnp.where(is_cond, velocity, other)
    uncond = jnp.where(is_cond, other, velocity)
    guided = uncond + GUIDE * (cond - uncond)
    denoised = noisy_latents - NOISE_LEVEL * guided
    pixels = (
        denoised * jnp.tile(latent_std, 4)[None, :] + jnp.tile(latent_mean, 4)[None, :]
    ).astype(jnp.bfloat16)
    block_start = (blk_index * seq_count + seq_index) * tok_rows
    local_slot = patch_order - block_start
    selector = (jnp.arange(tok_rows, dtype=jnp.int32)[:, None] == local_slot[None, :]).astype(
        jnp.bfloat16
    )
    placed = jnp.dot(selector, pixels, preferred_element_type=jnp.float32).astype(jnp.bfloat16)
    grid_cols = COLS_DEV * blk_count
    strip_rows = tok_rows // grid_cols
    strip = placed.reshape(1, strip_rows, grid_cols * placed.shape[1])
    received = lax.all_to_all(strip, "blk", split_axis=2, concat_axis=0, tiled=True)
    frame_count = received.shape[0]
    tile = (
        received.reshape(frame_count, strip_rows, COLS_DEV, 2, 2, ZCH)
        .transpose(0, 1, 3, 2, 4, 5)
        .reshape(frame_count, 2 * strip_rows, 2 * COLS_DEV, ZCH)
    )
    half = frame_count // 2
    leading = jnp.zeros((2,) + tile.shape[1:], jnp.bfloat16)
    timeline = jnp.concatenate([leading, tile], axis=0)
    window = lax.dynamic_slice_in_dim(timeline, cfg_index * half, half + 2, 0)
    framed = padded(window, (("seq", 1), ("blk", 2)), 1)
    tile_rows = 2 * strip_rows
    tile_cols = 2 * COLS_DEV
    columns = []
    for step_t in range(3):
        for step_y in range(3):
            for step_x in range(3):
                columns.append(
                    framed[
                        step_t : step_t + half,
                        step_y : step_y + tile_rows,
                        step_x : step_x + tile_cols,
                        :,
                    ]
                )
    stacked = jnp.concatenate(columns, axis=3).reshape(half * tile_rows * tile_cols, 27 * ZCH)
    kernel = conv_weight.reshape(27 * ZCH, conv_weight.shape[4])
    output = jnp.dot(stacked, kernel, preferred_element_type=jnp.float32) + conv_bias[None, :]
    return output.reshape(half, tile_rows, tile_cols, conv_weight.shape[4]).astype(jnp.bfloat16)


def pack_kernel(order_ref, own_ref, q_ref, k_ref, v_ref, head_ref, noisy_ref, *refs):
    sends, noise_ref, ordered_ref = refs[:-2], refs[-2], refs[-1]
    rows, width = sends[0].shape
    patch = noise_ref.shape[1]
    feat = width * HDIM // (2 * HDIM + patch)
    own = own_ref[0]
    slot = order_ref[...] - own * rows
    hit = lax.broadcasted_iota(jnp.int32, (rows, rows), 0) == slot
    selector = hit.astype(jnp.bfloat16)
    ordered = jnp.dot(selector, q_ref[...], preferred_element_type=jnp.float32)
    ordered_ref[...] = ordered.astype(jnp.bfloat16)
    for mask, send_ref in enumerate(sends):
        start = (own ^ mask) * feat
        cols = pl.ds(pl.multiple_of(start, HDIM), feat)
        send_ref[:, :feat] = ordered_ref[:, cols]
        send_ref[:, feat : 2 * feat] = k_ref[:, cols]
        for head in range(0, feat // HDIM, 2):
            both = []
            for step in range(2):
                at = pl.ds(pl.multiple_of(start + (head + step) * HDIM, HDIM), HDIM)
                both.append(
                    lax.dot_general(
                        v_ref[:, at],
                        head_ref[:, at],
                        (((1,), (1,)), ((), ())),
                        preferred_element_type=jnp.float32,
                    )
                )
            at = 2 * feat + head * patch
            send_ref[:, at : at + 2 * patch] = jnp.concatenate(both, axis=1).astype(jnp.bfloat16)
    noise_ref[...] = jnp.dot(
        hit.astype(jnp.float32),
        noisy_ref[...],
        preferred_element_type=jnp.float32,
        precision=lax.Precision.HIGHEST,
    )


def attend_kernel(place_ref, noise_ref, pick_ref, *refs):
    pieces, out_ref, acc_ref, qkv_ref = refs[:-3], refs[-3], refs[-2], refs[-1]
    tokens, width = qkv_ref.shape
    patch = acc_ref.shape[1]
    feat = width * HDIM // (2 * HDIM + patch)
    block = noise_ref.shape[0]
    for at, piece in enumerate(pieces):
        qkv_ref[at * block : (at + 1) * block, :] = piece[...]
    scale = 1.0 / math.sqrt(HDIM)
    wide_velocity = jnp.zeros((tokens, 2 * patch), jnp.float32)
    lane = lax.broadcasted_iota(jnp.int32, (tokens, 2 * patch), 1)
    for head in range(feat // HDIM):
        low = head * HDIM
        query = qkv_ref[:, low : low + HDIM]
        key = qkv_ref[:, feat + low : feat + low + HDIM]
        pair = 2 * feat + head // 2 * 2 * patch
        value = qkv_ref[:, pair : pair + 2 * patch]
        scores = (
            lax.dot_general(
                query, key, (((1,), (1,)), ((), ())), preferred_element_type=jnp.float32
            )
            * scale
        )
        expo = jnp.exp(scores - jnp.max(scores, axis=1, keepdims=True))
        total = jnp.sum(expo, axis=1, keepdims=True)
        mixed = jnp.dot(
            expo.astype(jnp.bfloat16), value, preferred_element_type=jnp.float32
        )
        mine = lane // patch == head % 2
        wide_velocity = wide_velocity + jnp.where(mine, mixed / total, 0.0)
    is_cond = place_ref[1] == 0
    factor = jnp.where(is_cond, -NOISE_LEVEL * GUIDE, -NOISE_LEVEL * (1.0 - GUIDE))
    velocity = (wide_velocity[:, :patch] + wide_velocity[:, patch:]) * factor
    for mask in range(len(pieces)):
        rows = pl.ds(pl.multiple_of((place_ref[0] ^ mask) * block, 8), block)
        acc_ref[rows, :] = velocity[mask * block : (mask + 1) * block]
    rows = pl.ds(pl.multiple_of(place_ref[0] * block, 8), block)
    acc_ref[rows, :] = acc_ref[rows, :] + noise_ref[...] * jnp.where(is_cond, 1.0, 0.0)
    share = acc_ref[...].astype(jnp.bfloat16)
    both = jnp.concatenate([share[: tokens // 2], share[tokens // 2 :]], axis=1)
    placed = jnp.dot(pick_ref[...], both, preferred_element_type=jnp.float32)
    placed = placed.astype(jnp.bfloat16)
    rows_each = out_ref.shape[2]
    for group in range(out_ref.shape[0]):
        piece = placed[group * rows_each : (group + 1) * rows_each]
        for core in range(out_ref.shape[1]):
            out_ref[group, core] = piece


def conv_kernel(
    place_ref,
    got_ref,
    std_ref,
    mean_ref,
    mesh_ref,
    big_ref,
    bias_ref,
    order_ref,
    out_ref,
):
    frames_out, tile_cols, tile_rows, channels = out_ref.shape
    wide = tile_cols // 2
    high = tile_rows // 2
    shares, rows, lanes = got_ref.shape
    summed = got_ref[0].astype(jnp.float32)
    for share in range(1, shares):
        summed = summed + got_ref[share].astype(jnp.float32)
    span = wide + 2
    tall = high + 2
    row = lax.broadcasted_iota(jnp.int32, (rows, lanes), 0)
    col_at = place_ref[0] * wide - 1 + row % span
    row_at = place_ref[1] * high - 1 + row // span % tall
    inside = (
        (col_at >= 0) & (col_at < place_ref[3]) & (row_at >= 0) & (row_at < place_ref[4])
    )
    pixels = jnp.where(inside, summed * std_ref[...] + mean_ref[...], 0.0)
    half = lanes // 2
    flat = jnp.concatenate([pixels[:, :half], pixels[:, half:]], axis=0)
    count = 2 * rows
    moved = pltpu.roll(flat, count - 1, 0)
    pairs = jnp.concatenate([flat, moved], axis=1).astype(jnp.bfloat16)
    wanted = mesh_ref[:, 0:1] + place_ref[2] * (frames_out * tall * span)
    hits = (lax.broadcasted_iota(jnp.int32, (mesh_ref.shape[0], count), 1) == wanted).astype(
        jnp.bfloat16
    )
    pieces = jnp.dot(hits, pairs, preferred_element_type=jnp.float32).astype(jnp.bfloat16)
    part = frames_out * high * wide
    part = (part + 15) // 16 * 16
    results = []
    for down in range(2):
        for right in range(2):
            which = down * 2 + right
            columns = []
            for step_t in range(3):
                for near in range(2):
                    at = (step_t * 3 + down + near) * 2 + right
                    columns.append(pieces[at * part : (at + 1) * part])
            stacked = jnp.concatenate(columns, axis=1)
            result = jnp.dot(stacked, big_ref[which], preferred_element_type=jnp.float32)
            results.append((result + bias_ref[...]).astype(jnp.bfloat16))
    together = jnp.concatenate(results, axis=0)
    final = jnp.dot(order_ref[...], together, preferred_element_type=jnp.float32)
    final = final.astype(jnp.bfloat16)
    for frame in range(frames_out):
        for x in range(tile_cols):
            at = (frame * tile_cols + x) * 8
            out_ref[frame, x] = final[at : at + tile_rows]


def tile_rows_of(seq_count, blk_count, frames, high, wide):
    grid_rows = seq_count * high
    grid_cols = blk_count * wide
    table = np.full((blk_count, seq_count, frames // 2, high + 2, wide + 2), -1, np.int32)
    for blk in range(blk_count):
        for seq in range(seq_count):
            for frame in range(frames // 2):
                for i in range(high + 2):
                    for w in range(wide + 2):
                        y = seq * high - 1 + i
                        x = blk * wide - 1 + w
                        if 0 <= y < grid_rows and 0 <= x < grid_cols:
                            table[blk, seq, frame, i, w] = (frame * grid_rows + y) * grid_cols + x
    return table.reshape(-1)


def window_rows(frames_out, high, wide):
    part = (frames_out * high * wide + 15) // 16 * 16
    table = np.full((3, 3, 2, part), -100000, np.int32)
    for step_t in range(3):
        for near in range(3):
            for right in range(2):
                for frame in range(frames_out):
                    for i in range(high):
                        for w in range(wide):
                            source = frame - 2 + step_t
                            at = (source * (high + 2) + i + near) * (wide + 2) + w + right
                            if source < 0:
                                at = (source * (high + 2) + i + near) * (wide + 2) + w + right
                            table[step_t, near, right, (frame * high + i) * wide + w] = at
    return table.reshape(-1, 1)


def output_order(frames_out, high, wide):
    part = (frames_out * high * wide + 15) // 16 * 16
    table = np.zeros((frames_out * 2 * wide * 8, 4 * part), np.float32)
    for frame in range(frames_out):
        for y in range(2 * high):
            for x in range(2 * wide):
                which = (y % 2) * 2 + x % 2
                source = which * part + (frame * high + y // 2) * wide + x // 2
                table[(frame * 2 * wide + x) * 8 + y, source] = 1.0
    return table


def exchange(pieces):
    seq_count = lax.axis_size("seq")
    blk_count = lax.axis_size("blk")

    def at(block):
        return block % seq_count * blk_count + block // seq_count

    got = [pieces[0]] + [None] * (len(pieces) - 1)
    near_first = sorted(range(1, len(pieces)), key=lambda mask: (mask.bit_count(), mask))
    for mask in near_first:
        pairs = [(at(i), at(i ^ mask)) for i in range(len(pieces))]
        got[mask] = lax.ppermute(pieces[mask], ("seq", "blk"), pairs)
    return got


def prepare_kernel(weight_ref, big_ref):
    big_ref[...] = jnp.zeros(big_ref.shape, big_ref.dtype)
    for down in range(2):
        for right in range(2):
            which = down * 2 + right
            for step_t in range(3):
                for step_y in range(3):
                    for step_x in range(3):
                        y = 1 - down + step_y
                        x = 1 - right + step_x
                        at = (step_t * 2 + y // 2) * 8 + (x // 2) * 4 + (y % 2) * 2 + x % 2
                        big_ref[which, at * ZCH : (at + 1) * ZCH, :] = weight_ref[
                            (step_t * 3 + step_y) * 3 + step_x
                        ]


def by_heads(
    queries,
    key_states,
    value_states,
    noisy_latents,
    patch_order,
    head_weight,
    latent_std,
    latent_mean,
    conv_weight,
    conv_bias,
):
    seq_count = lax.axis_size("seq")
    blk_count = lax.axis_size("blk")
    cfg_count = lax.axis_size("cfg")
    seq_index = lax.axis_index("seq")
    blk_index = lax.axis_index("blk")
    cfg_index = lax.axis_index("cfg")
    groups = seq_count * blk_count
    block = queries.shape[1]
    tokens = groups * block
    feat = queries.shape[2] // groups
    patch = noisy_latents.shape[1]
    width = 2 * feat + feat // HDIM * patch
    channels = conv_weight.shape[4]
    own = (blk_index * seq_count + seq_index).astype(jnp.int32)
    frames = blk_count
    grid_cols = COLS_DEV * blk_count
    high = block // grid_cols
    wide = COLS_DEV
    vmem = pl.BlockSpec(memory_space=pltpu.VMEM)
    smem = pl.BlockSpec(memory_space=pltpu.SMEM)
    *packed, noise = pl.pallas_call(
        pack_kernel,
        out_shape=tuple(pltpu.VMEM((block, width), jnp.bfloat16) for unused in range(groups))
        + (pltpu.VMEM((block, patch), jnp.float32),),
        in_specs=[vmem, smem] + [vmem] * 5,
        out_specs=(vmem,) * (groups + 1),
        scratch_shapes=[pltpu.VMEM(queries.shape[1:], jnp.bfloat16)],
    )(
        patch_order[None, :],
        own[None],
        queries[0],
        key_states[0],
        value_states[0],
        head_weight.T,
        noisy_latents,
    )
    received = [
        pltpu.with_memory_space_constraint(piece, pltpu.VMEM) for piece in exchange(packed)
    ]
    pick = (
        np.arange(tokens // 2)[None, :]
        == tile_rows_of(seq_count, blk_count, frames, high, wide)[:, None]
    )
    tile = frames // 2 * (high + 2) * (wide + 2)
    shares = pl.pallas_call(
        attend_kernel,
        out_shape=pltpu.VMEM((groups, cfg_count, tile, 2 * patch), jnp.bfloat16),
        in_specs=[smem] + [vmem] * (2 + groups),
        out_specs=vmem,
        scratch_shapes=[
            pltpu.VMEM((tokens, patch), jnp.float32),
            pltpu.VMEM((tokens, width), jnp.bfloat16),
        ],
    )(
        jnp.stack([own, cfg_index.astype(jnp.int32)]),
        pltpu.with_memory_space_constraint(noise, pltpu.VMEM),
        jnp.asarray(pick, jnp.bfloat16),
        *received,
    )
    got = lax.all_to_all(
        shares.reshape(groups * cfg_count, tile, 2 * patch),
        ("blk", "seq", "cfg"),
        split_axis=0,
        concat_axis=0,
        tiled=True,
    )
    place = jnp.stack(
        [blk_index, seq_index, cfg_index, jnp.int32(grid_cols), jnp.int32(seq_count * high)]
    ).astype(jnp.int32)
    frames_out = frames // cfg_count
    big = pl.pallas_call(
        prepare_kernel,
        out_shape=pltpu.VMEM((4, 48 * ZCH, channels), jnp.bfloat16),
        in_specs=[vmem],
        out_specs=vmem,
    )(conv_weight.reshape(27, ZCH, channels))
    features = pl.pallas_call(
        conv_kernel,
        out_shape=jax.ShapeDtypeStruct((frames_out, 2 * wide, 2 * high, channels), jnp.bfloat16),
        in_specs=[smem] + [vmem] * 7,
        out_specs=vmem,
    )(
        place,
        pltpu.with_memory_space_constraint(got, pltpu.VMEM),
        jnp.tile(latent_std, 2 * patch // ZCH)[None, :],
        jnp.tile(latent_mean, 2 * patch // ZCH)[None, :],
        jnp.asarray(window_rows(frames_out, high, wide)),
        pltpu.with_memory_space_constraint(big, pltpu.VMEM),
        conv_bias[None, :],
        jnp.asarray(output_order(frames_out, high, wide), jnp.bfloat16),
    )
    return features.transpose(0, 2, 1, 3)


def chosen(*arrays):
    groups = lax.axis_size("seq") * lax.axis_size("blk")
    heads = arrays[0].shape[2] // HDIM
    if heads % (2 * groups) == 0 and groups & (groups - 1) == 0:
        return by_heads(*arrays)
    return local(*arrays)


def solution(mesh):
    in_specs = (
        P("cfg", ("prompt", "blk", "seq"), None),
        P("cfg", ("prompt", "blk", "seq"), None),
        P("cfg", ("prompt", "blk", "seq"), None),
        P(("prompt", "blk", "seq"), None),
        P(("prompt", "blk", "seq")),
        P(),
        P(),
        P(),
        P(),
        P(),
    )
    out_specs = P(("prompt", "cfg"), "seq", "blk", None)
    return jax.shard_map(chosen, mesh=mesh, in_specs=in_specs, out_specs=out_specs, check_vma=False)
```

```python
import math

import jax
import jax.numpy as jnp
import numpy as np
from jax import lax
from jax.experimental import pallas as pl
from jax.experimental.pallas import tpu as pltpu
from jax.sharding import PartitionSpec as P

HDIM = 128
ZCH = 16
COLS_DEV = 3


GUIDE = 5.0
NOISE_LEVEL = 0.5


def partner(array, axis, apart):
    return lax.ppermute(array, axis, [(i, i ^ 1 << apart) for i in range(lax.axis_size(axis))])


def padded(array, sides, width):
    for axis, dim in sides:
        devices, length = (lax.axis_size(axis), array.shape[dim])
        up = [(i, (i + 1) % devices) for i in range(devices - 1)]
        down = [(j, i) for i, j in up]
        last = lax.slice_in_dim(array, length - width, length, axis=dim)
        first = lax.slice_in_dim(array, 0, width, axis=dim)
        before = lax.ppermute(last, axis, up)
        after = lax.ppermute(first, axis, down)
        array = jnp.concatenate([before, array, after], axis=dim)
    return array


def fold_keys(carry, piece, grouped, block):
    keys_piece, values_piece = piece
    heads = grouped.shape[1]
    count = keys_piece.shape[0] // block
    key_blocks = keys_piece.reshape(count, block, heads, HDIM)
    value_blocks = values_piece.reshape(count, block, heads, HDIM)
    scale = 1.0 / math.sqrt(HDIM)

    def one_block(state, pair):
        top, total, acc = state
        key_block, value_block = pair
        scores = (
            jnp.einsum("qhd,khd->hqk", grouped, key_block, preferred_element_type=jnp.float32)
            * scale
        )
        new_top = jnp.maximum(top, jnp.max(scores, axis=2))
        expo = jnp.exp(scores - new_top[:, :, None])
        factor = jnp.exp(top - new_top)
        total = total * factor + jnp.sum(expo, axis=2)
        weights = expo.astype(jnp.bfloat16)
        update = jnp.einsum(
            "hqk,khd->qhd", weights, value_block, preferred_element_type=jnp.float32
        )
        acc = acc * factor.T[:, :, None] + update
        return ((new_top, total, acc), None)

    state, unused = lax.scan(one_block, carry, (key_blocks, value_blocks))
    return state


def start_for(rows, heads):
    return (
        jnp.full((heads, rows), -1e30, jnp.float32),
        jnp.zeros((heads, rows), jnp.float32),
        jnp.zeros((rows, heads, HDIM), jnp.float32),
    )


def finish(state):
    top, total, acc = state
    rows = acc.shape[0]
    return (acc / total.T[:, :, None]).astype(jnp.bfloat16).reshape(rows, acc.shape[1] * HDIM)


def local(
    queries,
    key_states,
    value_states,
    noisy_latents,
    patch_order,
    head_weight,
    latent_std,
    latent_mean,
    conv_weight,
    conv_bias,
):
    seq_count = lax.axis_size("seq")
    blk_count = lax.axis_size("blk")
    seq_index = lax.axis_index("seq")
    blk_index = lax.axis_index("blk")
    cfg_index = lax.axis_index("cfg")
    tok_rows = queries.shape[1]
    own_query = queries[0]
    own_keys = key_states[0]
    own_values = value_states[0]
    local_query, local_keys, local_values = (
        lax.all_to_all(own_query, "seq", split_axis=1, concat_axis=0, tiled=True),
        lax.all_to_all(own_keys, "seq", split_axis=1, concat_axis=0, tiled=True),
        lax.all_to_all(own_values, "seq", split_axis=1, concat_axis=0, tiled=True),
    )
    frame_rows = local_query.shape[0]
    half_feat = local_query.shape[1] // 2
    is_even = blk_index % 2 == 0

    def keep_give(whole):
        first = whole[:, :half_feat]
        second = whole[:, half_feat:]
        return (jnp.where(is_even, first, second), jnp.where(is_even, second, first))

    keep_q, give_q = keep_give(local_query)
    keep_k, give_k = keep_give(local_keys)
    keep_v, give_v = keep_give(local_values)
    got_q, got_k, got_v = partner((give_q, give_k, give_v), "blk", 0)

    def in_order(kept, got):
        return jnp.where(
            is_even, jnp.concatenate([kept, got], axis=0), jnp.concatenate([got, kept], axis=0)
        )

    pair_query = in_order(keep_q, got_q)
    held_keys = in_order(keep_k, got_k)
    held_values = in_order(keep_v, got_v)
    heads = half_feat // HDIM
    grouped = pair_query.reshape(2 * frame_rows, heads, HDIM)
    state = fold_keys(
        start_for(2 * frame_rows, heads), (held_keys, held_values), grouped, frame_rows
    )
    for bit in range(1, blk_count.bit_length() - 1):
        far_keys, far_values = partner((held_keys, held_values), "blk", bit)
        state = fold_keys(state, (far_keys, far_values), grouped, frame_rows)
        held_keys = jnp.concatenate([held_keys, far_keys], axis=0)
        held_values = jnp.concatenate([held_values, far_values], axis=0)
    paired_out = finish(state)
    mine_rows = jnp.where(is_even, paired_out[:frame_rows], paired_out[frame_rows:])
    their_rows = jnp.where(is_even, paired_out[frame_rows:], paired_out[:frame_rows])
    returned = partner(their_rows, "blk", 0)
    attended = jnp.where(
        is_even,
        jnp.concatenate([mine_rows, returned], axis=1),
        jnp.concatenate([returned, mine_rows], axis=1),
    )
    token_features = lax.all_to_all(attended, "seq", split_axis=0, concat_axis=1, tiled=True)
    velocity = jnp.dot(token_features, head_weight, preferred_element_type=jnp.float32)
    other = partner(velocity, "cfg", 0)
    is_cond = cfg_index == 0
    cond = jnp.where(is_cond, velocity, other)
    uncond = jnp.where(is_cond, other, velocity)
    guided = uncond + GUIDE * (cond - uncond)
    denoised = noisy_latents - NOISE_LEVEL * guided
    pixels = (
        denoised * jnp.tile(latent_std, 4)[None, :] + jnp.tile(latent_mean, 4)[None, :]
    ).astype(jnp.bfloat16)
    block_start = (blk_index * seq_count + seq_index) * tok_rows
    local_slot = patch_order - block_start
    selector = (jnp.arange(tok_rows, dtype=jnp.int32)[:, None] == local_slot[None, :]).astype(
        jnp.bfloat16
    )
    placed = jnp.dot(selector, pixels, preferred_element_type=jnp.float32).astype(jnp.bfloat16)
    grid_cols = COLS_DEV * blk_count
    strip_rows = tok_rows // grid_cols
    strip = placed.reshape(1, strip_rows, grid_cols * placed.shape[1])
    received = lax.all_to_all(strip, "blk", split_axis=2, concat_axis=0, tiled=True)
    frame_count = received.shape[0]
    tile = (
        received.reshape(frame_count, strip_rows, COLS_DEV, 2, 2, ZCH)
        .transpose(0, 1, 3, 2, 4, 5)
        .reshape(frame_count, 2 * strip_rows, 2 * COLS_DEV, ZCH)
    )
    half = frame_count // 2
    leading = jnp.zeros((2,) + tile.shape[1:], jnp.bfloat16)
    timeline = jnp.concatenate([leading, tile], axis=0)
    window = lax.dynamic_slice_in_dim(timeline, cfg_index * half, half + 2, 0)
    framed = padded(window, (("seq", 1), ("blk", 2)), 1)
    tile_rows = 2 * strip_rows
    tile_cols = 2 * COLS_DEV
    columns = []
    for step_t in range(3):
        for step_y in range(3):
            for step_x in range(3):
                columns.append(
                    framed[
                        step_t : step_t + half,
                        step_y : step_y + tile_rows,
                        step_x : step_x + tile_cols,
                        :,
                    ]
                )
    stacked = jnp.concatenate(columns, axis=3).reshape(half * tile_rows * tile_cols, 27 * ZCH)
    kernel = conv_weight.reshape(27 * ZCH, conv_weight.shape[4])
    output = jnp.dot(stacked, kernel, preferred_element_type=jnp.float32) + conv_bias[None, :]
    return output.reshape(half, tile_rows, tile_cols, conv_weight.shape[4]).astype(jnp.bfloat16)


def pack_kernel(order_ref, own_ref, q_ref, k_ref, v_ref, head_ref, noisy_ref, *refs):
    sends, noise_ref, ordered_ref = refs[:-2], refs[-2], refs[-1]
    rows, width = sends[0].shape
    patch = noise_ref.shape[1]
    feat = width * HDIM // (2 * HDIM + patch)
    own = own_ref[0]
    slot = order_ref[...] - own * rows
    hit = lax.broadcasted_iota(jnp.int32, (rows, rows), 0) == slot
    selector = hit.astype(jnp.bfloat16)
    ordered = jnp.dot(selector, q_ref[...], preferred_element_type=jnp.float32)
    ordered_ref[...] = ordered.astype(jnp.bfloat16)
    for mask, send_ref in enumerate(sends):
        start = (own ^ mask) * feat
        cols = pl.ds(pl.multiple_of(start, HDIM), feat)
        send_ref[:, :feat] = ordered_ref[:, cols]
        send_ref[:, feat : 2 * feat] = k_ref[:, cols]
        for head in range(0, feat // HDIM, 2):
            both = []
            for step in range(2):
                at = pl.ds(pl.multiple_of(start + (head + step) * HDIM, HDIM), HDIM)
                both.append(
                    lax.dot_general(
                        v_ref[:, at],
                        head_ref[:, at],
                        (((1,), (1,)), ((), ())),
                        preferred_element_type=jnp.float32,
                    )
                )
            at = 2 * feat + head * patch
            send_ref[:, at : at + 2 * patch] = jnp.concatenate(both, axis=1).astype(jnp.bfloat16)
    noise_ref[...] = jnp.dot(
        hit.astype(jnp.float32),
        noisy_ref[...],
        preferred_element_type=jnp.float32,
        precision=lax.Precision.HIGHEST,
    )


def attend_kernel(place_ref, noise_ref, pick_ref, *refs):
    pieces, out_ref, acc_ref, qkv_ref = refs[:-3], refs[-3], refs[-2], refs[-1]
    tokens, width = qkv_ref.shape
    patch = acc_ref.shape[1]
    feat = width * HDIM // (2 * HDIM + patch)
    block = noise_ref.shape[0]
    for at, piece in enumerate(pieces):
        qkv_ref[at * block : (at + 1) * block, :] = piece[...]
    scale = 1.0 / math.sqrt(HDIM)
    wide_velocity = jnp.zeros((tokens, 2 * patch), jnp.float32)
    lane = lax.broadcasted_iota(jnp.int32, (tokens, 2 * patch), 1)
    for head in range(feat // HDIM):
        low = head * HDIM
        query = qkv_ref[:, low : low + HDIM]
        key = qkv_ref[:, feat + low : feat + low + HDIM]
        pair = 2 * feat + head // 2 * 2 * patch
        value = qkv_ref[:, pair : pair + 2 * patch]
        scores = (
            lax.dot_general(
                query, key, (((1,), (1,)), ((), ())), preferred_element_type=jnp.float32
            )
            * scale
        )
        expo = jnp.exp(scores - jnp.max(scores, axis=1, keepdims=True))
        total = jnp.sum(expo, axis=1, keepdims=True)
        mixed = jnp.dot(
            expo.astype(jnp.bfloat16), value, preferred_element_type=jnp.float32
        )
        mine = lane // patch == head % 2
        wide_velocity = wide_velocity + jnp.where(mine, mixed * (1.0 / total), 0.0)
    is_cond = place_ref[1] == 0
    factor = jnp.where(is_cond, -NOISE_LEVEL * GUIDE, -NOISE_LEVEL * (1.0 - GUIDE))
    velocity = (wide_velocity[:, :patch] + wide_velocity[:, patch:]) * factor
    for mask in range(len(pieces)):
        rows = pl.ds(pl.multiple_of((place_ref[0] ^ mask) * block, 8), block)
        acc_ref[rows, :] = velocity[mask * block : (mask + 1) * block]
    rows = pl.ds(pl.multiple_of(place_ref[0] * block, 8), block)
    acc_ref[rows, :] = acc_ref[rows, :] + noise_ref[...] * jnp.where(is_cond, 1.0, 0.0)
    share = acc_ref[...].astype(jnp.bfloat16)
    both = jnp.concatenate([share[: tokens // 2], share[tokens // 2 :]], axis=1)
    placed = jnp.dot(pick_ref[...], both, preferred_element_type=jnp.float32)
    placed = placed.astype(jnp.bfloat16)
    rows_each = out_ref.shape[2]
    for group in range(out_ref.shape[0]):
        piece = placed[group * rows_each : (group + 1) * rows_each]
        for core in range(out_ref.shape[1]):
            out_ref[group, core] = piece


def conv_kernel(
    place_ref,
    got_ref,
    std_ref,
    mean_ref,
    mesh_ref,
    big_ref,
    bias_ref,
    order_ref,
    out_ref,
):
    frames_out, tile_cols, tile_rows, channels = out_ref.shape
    wide = tile_cols // 2
    high = tile_rows // 2
    shares, rows, lanes = got_ref.shape
    summed = got_ref[0].astype(jnp.float32)
    for share in range(1, shares):
        summed = summed + got_ref[share].astype(jnp.float32)
    span = wide + 2
    tall = high + 2
    row = lax.broadcasted_iota(jnp.int32, (rows, lanes), 0)
    col_at = place_ref[0] * wide - 1 + row % span
    row_at = place_ref[1] * high - 1 + row // span % tall
    inside = (
        (col_at >= 0) & (col_at < place_ref[3]) & (row_at >= 0) & (row_at < place_ref[4])
    )
    pixels = jnp.where(inside, summed * std_ref[...] + mean_ref[...], 0.0)
    half = lanes // 2
    flat = jnp.concatenate([pixels[:, :half], pixels[:, half:]], axis=0)
    count = 2 * rows
    moved = pltpu.roll(flat, count - 1, 0)
    pairs = jnp.concatenate([flat, moved], axis=1).astype(jnp.bfloat16)
    wanted = mesh_ref[:, 0:1] + place_ref[2] * (frames_out * tall * span)
    hits = (lax.broadcasted_iota(jnp.int32, (mesh_ref.shape[0], count), 1) == wanted).astype(
        jnp.bfloat16
    )
    pieces = jnp.dot(hits, pairs, preferred_element_type=jnp.float32).astype(jnp.bfloat16)
    part = frames_out * high * wide
    part = (part + 15) // 16 * 16
    results = []
    for down in range(2):
        for right in range(2):
            which = down * 2 + right
            columns = []
            for step_t in range(3):
                for near in range(2):
                    at = (step_t * 3 + down + near) * 2 + right
                    columns.append(pieces[at * part : (at + 1) * part])
            stacked = jnp.concatenate(columns, axis=1)
            result = jnp.dot(stacked, big_ref[which], preferred_element_type=jnp.float32)
            results.append((result + bias_ref[...]).astype(jnp.bfloat16))
    together = jnp.concatenate(results, axis=0)
    final = jnp.dot(order_ref[...], together, preferred_element_type=jnp.float32)
    final = final.astype(jnp.bfloat16)
    for frame in range(frames_out):
        for x in range(tile_cols):
            at = (frame * tile_cols + x) * 8
            out_ref[frame, x] = final[at : at + tile_rows]


def tile_rows_of(seq_count, blk_count, frames, high, wide):
    grid_rows = seq_count * high
    grid_cols = blk_count * wide
    table = np.full((blk_count, seq_count, frames // 2, high + 2, wide + 2), -1, np.int32)
    for blk in range(blk_count):
        for seq in range(seq_count):
            for frame in range(frames // 2):
                for i in range(high + 2):
                    for w in range(wide + 2):
                        y = seq * high - 1 + i
                        x = blk * wide - 1 + w
                        if 0 <= y < grid_rows and 0 <= x < grid_cols:
                            table[blk, seq, frame, i, w] = (frame * grid_rows + y) * grid_cols + x
    return table.reshape(-1)


def window_rows(frames_out, high, wide):
    part = (frames_out * high * wide + 15) // 16 * 16
    table = np.full((3, 3, 2, part), -100000, np.int32)
    for step_t in range(3):
        for near in range(3):
            for right in range(2):
                for frame in range(frames_out):
                    for i in range(high):
                        for w in range(wide):
                            source = frame - 2 + step_t
                            at = (source * (high + 2) + i + near) * (wide + 2) + w + right
                            if source < 0:
                                at = (source * (high + 2) + i + near) * (wide + 2) + w + right
                            table[step_t, near, right, (frame * high + i) * wide + w] = at
    return table.reshape(-1, 1)


def output_order(frames_out, high, wide):
    part = (frames_out * high * wide + 15) // 16 * 16
    table = np.zeros((frames_out * 2 * wide * 8, 4 * part), np.float32)
    for frame in range(frames_out):
        for y in range(2 * high):
            for x in range(2 * wide):
                which = (y % 2) * 2 + x % 2
                source = which * part + (frame * high + y // 2) * wide + x // 2
                table[(frame * 2 * wide + x) * 8 + y, source] = 1.0
    return table


def exchange(pieces):
    seq_count = lax.axis_size("seq")
    blk_count = lax.axis_size("blk")

    def at(block):
        return block % seq_count * blk_count + block // seq_count

    got = [pieces[0]] + [None] * (len(pieces) - 1)
    near_first = sorted(range(1, len(pieces)), key=lambda mask: (mask.bit_count(), mask))
    for mask in near_first:
        pairs = [(at(i), at(i ^ mask)) for i in range(len(pieces))]
        got[mask] = lax.ppermute(pieces[mask], ("seq", "blk"), pairs)
    return got


def prepare_kernel(weight_ref, big_ref):
    big_ref[...] = jnp.zeros(big_ref.shape, big_ref.dtype)
    for down in range(2):
        for right in range(2):
            which = down * 2 + right
            for step_t in range(3):
                for step_y in range(3):
                    for step_x in range(3):
                        y = 1 - down + step_y
                        x = 1 - right + step_x
                        at = (step_t * 2 + y // 2) * 8 + (x // 2) * 4 + (y % 2) * 2 + x % 2
                        big_ref[which, at * ZCH : (at + 1) * ZCH, :] = weight_ref[
                            (step_t * 3 + step_y) * 3 + step_x
                        ]


def by_heads(
    queries,
    key_states,
    value_states,
    noisy_latents,
    patch_order,
    head_weight,
    latent_std,
    latent_mean,
    conv_weight,
    conv_bias,
):
    seq_count = lax.axis_size("seq")
    blk_count = lax.axis_size("blk")
    cfg_count = lax.axis_size("cfg")
    seq_index = lax.axis_index("seq")
    blk_index = lax.axis_index("blk")
    cfg_index = lax.axis_index("cfg")
    groups = seq_count * blk_count
    block = queries.shape[1]
    tokens = groups * block
    feat = queries.shape[2] // groups
    patch = noisy_latents.shape[1]
    width = 2 * feat + feat // HDIM * patch
    channels = conv_weight.shape[4]
    own = (blk_index * seq_count + seq_index).astype(jnp.int32)
    frames = blk_count
    grid_cols = COLS_DEV * blk_count
    high = block // grid_cols
    wide = COLS_DEV
    vmem = pl.BlockSpec(memory_space=pltpu.VMEM)
    smem = pl.BlockSpec(memory_space=pltpu.SMEM)
    *packed, noise = pl.pallas_call(
        pack_kernel,
        out_shape=tuple(pltpu.VMEM((block, width), jnp.bfloat16) for unused in range(groups))
        + (pltpu.VMEM((block, patch), jnp.float32),),
        in_specs=[vmem, smem] + [vmem] * 5,
        out_specs=(vmem,) * (groups + 1),
        scratch_shapes=[pltpu.VMEM(queries.shape[1:], jnp.bfloat16)],
    )(
        patch_order[None, :],
        own[None],
        queries[0],
        key_states[0],
        value_states[0],
        head_weight.T,
        noisy_latents,
    )
    received = [
        pltpu.with_memory_space_constraint(piece, pltpu.VMEM) for piece in exchange(packed)
    ]
    pick = (
        np.arange(tokens // 2)[None, :]
        == tile_rows_of(seq_count, blk_count, frames, high, wide)[:, None]
    )
    tile = frames // 2 * (high + 2) * (wide + 2)
    shares = pl.pallas_call(
        attend_kernel,
        out_shape=pltpu.VMEM((groups, cfg_count, tile, 2 * patch), jnp.bfloat16),
        in_specs=[smem] + [vmem] * (2 + groups),
        out_specs=vmem,
        scratch_shapes=[
            pltpu.VMEM((tokens, patch), jnp.float32),
            pltpu.VMEM((tokens, width), jnp.bfloat16),
        ],
    )(
        jnp.stack([own, cfg_index.astype(jnp.int32)]),
        pltpu.with_memory_space_constraint(noise, pltpu.VMEM),
        jnp.asarray(pick, jnp.bfloat16),
        *received,
    )
    got = lax.all_to_all(
        shares.reshape(groups * cfg_count, tile, 2 * patch),
        ("blk", "seq", "cfg"),
        split_axis=0,
        concat_axis=0,
        tiled=True,
    )
    place = jnp.stack(
        [blk_index, seq_index, cfg_index, jnp.int32(grid_cols), jnp.int32(seq_count * high)]
    ).astype(jnp.int32)
    frames_out = frames // cfg_count
    big = pl.pallas_call(
        prepare_kernel,
        out_shape=pltpu.VMEM((4, 48 * ZCH, channels), jnp.bfloat16),
        in_specs=[vmem],
        out_specs=vmem,
    )(conv_weight.reshape(27, ZCH, channels))
    features = pl.pallas_call(
        conv_kernel,
        out_shape=jax.ShapeDtypeStruct((frames_out, 2 * wide, 2 * high, channels), jnp.bfloat16),
        in_specs=[smem] + [vmem] * 7,
        out_specs=vmem,
    )(
        place,
        pltpu.with_memory_space_constraint(got, pltpu.VMEM),
        jnp.tile(latent_std, 2 * patch // ZCH)[None, :],
        jnp.tile(latent_mean, 2 * patch // ZCH)[None, :],
        jnp.asarray(window_rows(frames_out, high, wide)),
        pltpu.with_memory_space_constraint(big, pltpu.VMEM),
        conv_bias[None, :],
        jnp.asarray(output_order(frames_out, high, wide), jnp.bfloat16),
    )
    return features.transpose(0, 2, 1, 3)


def chosen(*arrays):
    groups = lax.axis_size("seq") * lax.axis_size("blk")
    heads = arrays[0].shape[2] // HDIM
    if heads % (2 * groups) == 0 and groups & (groups - 1) == 0:
        return by_heads(*arrays)
    return local(*arrays)


def solution(mesh):
    in_specs = (
        P("cfg", ("prompt", "blk", "seq"), None),
        P("cfg", ("prompt", "blk", "seq"), None),
        P("cfg", ("prompt", "blk", "seq"), None),
        P(("prompt", "blk", "seq"), None),
        P(("prompt", "blk", "seq")),
        P(),
        P(),
        P(),
        P(),
        P(),
    )
    out_specs = P(("prompt", "cfg"), "seq", "blk", None)
    return jax.shard_map(chosen, mesh=mesh, in_specs=in_specs, out_specs=out_specs, check_vma=False)
```
